256 devices in a mesh: row: 32 (over y, z), col: 8 (over x, core).
Axes of the slice: x: 4, y: 4, z: 8, core: 2. Of those that a mesh axis runs over, the one named last changes fastest.
Arguments:
- tile_u: bfloat16 [3, 32, 2, 8, 512, 128], P(None, 'row', None, 'col'), may hold values from -6 to 6
- tile_v: bfloat16 [3, 32, 2, 8, 512, 128], P(None, 'row', None, 'col'), may hold values from -6 to 6
- tile_ranks: int32 [3, 32, 2, 8], P(None, 'row', None, 'col'), may hold values from 16 to 128
- lower_inverse: bfloat16 [2, 512, 512], replicated, as said below
- upper_inverse: bfloat16 [2, 512, 512], replicated, as said below
- row_order: int32 [2, 512], replicated, may hold values from 0 to 511, each once within a row
- sketch: bfloat16 [512, 128], replicated, may hold values from -0.25 to 0.25
Outputs:
- new_u: bfloat16 [3, 32, 2, 8, 512, 128], P(None, 'row', None, 'col')
- new_v: bfloat16 [3, 32, 2, 8, 512, 128], P(None, 'row', None, 'col')
The draws below stay inside these ranges and needn't reach their ends.
Inputs may be any that keep to these rules, and one draw needn't show every extreme that they name: Each row of row_order names every number of 0 to 511 once. Each lower_inverse[k] is lower triangular with a unit diagonal. Each upper_inverse[k] is upper triangular with a positive diagonal.
All inputs are finite; a program needn't handle non-finite values.
Results may differ from the reference program's by a relative error of at most 0.03.
Values may be sent and summed in bfloat16 or wider, within the bound.
No kernel may reach another device: no remote copies, remote signals or barrier semaphores. Data moves between devices by JAX's collectives and lax.ppermute only.
A program may use at most 64 MiB of HBM per device.

```python
import math
import jax
import jax.numpy as jnp
from jax import lax

B = 512
R = 128
PANELS = 2
TR_DEV = 3
TC_DEV = 2
N_ROW = 32
N_COL = 8


def draw_lower_inverse(key, part):
    noise = jax.random.normal(key, (PANELS, B, B), jnp.float32)
    strict = jnp.tril(noise, -1) * B ** (-0.5)
    return (strict + jnp.eye(B, dtype=jnp.float32)).astype(jnp.bfloat16)


def draw_upper_inverse(key, part):
    first_key, second_key = jax.random.split(jax.random.fold_in(key, 7))
    noise = jax.random.normal(first_key, (PANELS, B, B), jnp.float32)
    diagonal = jnp.exp(jax.random.uniform(second_key, (PANELS, B), jnp.float32, math.log(0.5), math.log(2.0)))
    matrix = jnp.triu(noise, 1) * B ** (-0.5) + diagonal[:, :, None] * jnp.eye(B, dtype=jnp.float32)
    return (matrix * B ** (-0.5)).astype(jnp.bfloat16)


def with_ends(values, key, low, largest):
    longest = values.shape.index(max(values.shape))
    spots = []
    for shift in (0, 1):
        where = [jax.random.randint(jax.random.fold_in(key, axis), (), 0, length) for axis, length in enumerate(values.shape)]
        where[longest] = (where[longest] + shift) % values.shape[longest]
        spots.append(tuple(where))
    return values.at[spots[0]].set(low).at[spots[1]].set(largest)


def level_of(rng, shape, cuts, least, top_value):
    def one(position, blocks):
        steps = jax.random.uniform(jax.random.fold_in(jax.random.fold_in(rng, 6), position), (blocks,), jnp.float32, least / len(cuts), top_value / len(cuts))
        return jnp.repeat(jnp.exp(steps), shape[position] // blocks).reshape((-1,) + (1,) * (len(shape) - position - 1))

    factor_of = one(*cuts[0])
    for cut in cuts[1:]:
        factor_of = factor_of * one(*cut)
    return factor_of


def scatter_about(stream_key, shape, scale, bound, cuts=(), held_as=jnp.bfloat16):
    drawn = jax.random.normal(stream_key, shape, jnp.float32) * scale
    if len(cuts) > 0:
        drawn = level_of(stream_key, shape, cuts, -0.22, 0.18) * drawn
    return jnp.clip(drawn, min=-bound, max=bound).astype(held_as)


def setup_inputs(seed: int = 0) -> dict:
    key_of = jax.random.split(jax.random.key(seed), 8)
    tile_u = scatter_about(key_of[0], (TR_DEV, N_ROW, TC_DEV, N_COL, B, R), 1.0, 6.0, ((1, 32), (3, 8)))
    tile_v = scatter_about(key_of[1], (TR_DEV, N_ROW, TC_DEV, N_COL, B, R), 1.0, 6.0, ((1, 32), (3, 8)))
    tile_ranks = with_ends(jax.random.randint(key_of[2], (TR_DEV, N_ROW, TC_DEV, N_COL), R // 8, R + 1), jax.random.fold_in(key_of[2], 1), R // 8, R).astype(jnp.int32)
    lower_inverse = draw_lower_inverse(jax.random.fold_in(key_of[7], 71), 0)
    upper_inverse = draw_upper_inverse(jax.random.fold_in(key_of[7], 71), 0)
    row_order = jax.vmap(lambda own: jax.random.permutation(own, B))(jax.random.split(key_of[5], PANELS)).reshape((PANELS, B)).astype(jnp.int32)
    sketch = scatter_about(key_of[6], (B, R), B ** -0.5, 0.25)
    return dict(tile_u=tile_u, tile_v=tile_v, tile_ranks=tile_ranks, lower_inverse=lower_inverse, upper_inverse=upper_inverse, row_order=row_order, sketch=sketch)


HIGHEST = lax.Precision.HIGHEST

def compress(tile_uf, tile_vf, left_u, coupling, top_v, keep_cols, sketch):
    rank_width = tile_uf.shape[-1]
    tile_size = tile_uf.shape[-2]
    product = jnp.einsum('...br,...rs->...bs', left_u.astype(jnp.float32), coupling.astype(jnp.float32), precision=HIGHEST)
    update = (product * rank_width ** (-0.5)).astype(jnp.bfloat16)
    stacked_left = jnp.concatenate([tile_uf, -update], axis=-1).astype(jnp.float32)
    stacked_right = jnp.concatenate([tile_vf, top_v], axis=-1).astype(jnp.float32)
    probe_mat = jnp.einsum('...bt,br->...tr', stacked_right, sketch.astype(jnp.float32), precision=HIGHEST)
    sample = jnp.einsum('...bt,...tr->...br', stacked_left, probe_mat, precision=HIGHEST) * keep_cols[..., None, :]
    gram_matrix = jnp.einsum('...br,...bs->...rs', sample, sample, precision=HIGHEST)
    gram_matrix = gram_matrix + (1.0 - keep_cols)[..., :, None] * jnp.eye(rank_width, dtype=jnp.float32)
    factor = jnp.linalg.cholesky(gram_matrix)
    solved = lax.linalg.triangular_solve(factor, jnp.swapaxes(sample, -1, -2), left_side=True, lower=True)
    new_basis = jnp.swapaxes(solved, -1, -2)
    weights_q = jnp.einsum('...bt,...br->...tr', stacked_left, new_basis, precision=HIGHEST)
    fresh_v = jnp.einsum('...bt,...tr->...br', stacked_right, weights_q, precision=HIGHEST)
    return ((new_basis * tile_size ** 0.5).astype(jnp.bfloat16), (fresh_v * tile_size ** (-0.5)).astype(jnp.bfloat16))

def reference(tile_u, tile_v, tile_ranks, lower_inverse, upper_inverse, row_order, sketch):
    tile_rows = TR_DEV * N_ROW
    tile_cols = TC_DEV * N_COL
    shape_four = (tile_rows, tile_cols, B, R)
    tile_rank = tile_ranks.reshape(tile_rows, tile_cols)
    keep_flags_mask = jnp.arange(R, dtype=jnp.int32)[None, None, :] < tile_rank[:, :, None]
    keep_cols = keep_flags_mask.astype(jnp.float32)
    keep_half = keep_flags_mask.astype(jnp.bfloat16)[:, :, None, :]
    factor_left_bases = tile_u.reshape(shape_four) * keep_half
    factors_v = tile_v.reshape(shape_four) * keep_half
    row_ids = jnp.arange(tile_rows, dtype=jnp.int32)
    col_ids = jnp.arange(tile_cols, dtype=jnp.int32)
    for panel in range(PANELS):
        permuted = jnp.take(factor_left_bases[panel], row_order[panel], axis=1)
        turned_u = jnp.einsum('ab,mbr->mar', lower_inverse[panel].astype(jnp.float32), permuted.astype(jnp.float32), precision=HIGHEST).astype(jnp.bfloat16)
        top_u = jnp.where((col_ids > panel)[:, None, None], turned_u, factor_left_bases[panel])
        transposed_right_basis = jnp.einsum('ba,lbr->lar', upper_inverse[panel].astype(jnp.float32), factors_v[:, panel].astype(jnp.float32), precision=HIGHEST)
        transposed_right_basis = (transposed_right_basis * B ** 0.5).astype(jnp.bfloat16)
        left_right_basis = jnp.where((row_ids > panel)[:, None, None], transposed_right_basis, factors_v[:, panel])
        factor_left_bases = factor_left_bases.at[panel].set(top_u)
        factors_v = factors_v.at[:, panel].set(left_right_basis)
        top_v = factors_v[panel]
        left_u = factor_left_bases[:, panel]

        def single_row_slice(row_item, panel=panel, top_u=top_u, top_v=top_v):
            row_u, row_v, row_left_u, row_left_v, row_keep, row_id = row_item
            coupling = jnp.einsum('br,mbs->mrs', row_left_v.astype(jnp.float32), top_u.astype(jnp.float32), precision=HIGHEST)
            coupling = (coupling * B ** (-0.5)).astype(jnp.bfloat16)
            left_full = jnp.broadcast_to(row_left_u[None], row_u.shape)
            fresh_u, fresh_v = compress(row_u, row_v, left_full, coupling, top_v, row_keep, sketch)
            chosen = ((row_id > panel) & (col_ids > panel))[:, None, None]
            return (jnp.where(chosen, fresh_u, row_u), jnp.where(chosen, fresh_v, row_v))
        factor_left_bases, factors_v = lax.map(single_row_slice, (factor_left_bases, factors_v, left_u, left_right_basis, keep_cols, row_ids))
    return (factor_left_bases.reshape(tile_u.shape), factors_v.reshape(tile_v.shape))
```

```python
import functools

import jax
import jax.numpy as jnp
from jax import lax
from jax.experimental import pallas as pl
from jax.experimental.pallas import tpu as pltpu
from jax.sharding import Mesh
from jax.sharding import PartitionSpec as P

PANELS = 2
STEP = 16
F32 = jnp.float32
BF16 = jnp.bfloat16


def dot_nn(a, b):
    return lax.dot_general(a, b, (((1,), (0,)), ((), ())), preferred_element_type=F32)


def dot_nt(a, b):
    return lax.dot_general(a, b, (((1,), (1,)), ((), ())), preferred_element_type=F32)


def dot_tn(a, b):
    return lax.dot_general(a, b, (((0,), (0,)), ((), ())), preferred_element_type=F32)


def halves(x):
    high = x.astype(BF16)
    return high, (x - high.astype(F32)).astype(BF16)


def thirds(x):
    high = x.astype(BF16)
    rest = x - high.astype(F32)
    middle = rest.astype(BF16)
    return high, middle, (rest - middle.astype(F32)).astype(BF16)


def factor_block(rows, start, lane, sub):
    count = len(rows) * 8
    cols = [
        [
            jnp.broadcast_to(rows[h][:, start + c : start + c + 1], (8, 128))
            if c < 8 * (h + 1)
            else None
            for h in range(len(rows))
        ]
        for c in range(count)
    ]
    panel = []
    for h in range(len(rows)):
        own = (lane >= start) & (lane < start + count)
        unit = (lane == sub + (start + 8 * h)).astype(F32)
        panel.append(jnp.where(own, unit, rows[h]))
    done = [jnp.zeros((8, 128), F32) for _ in rows]
    for p in range(count):
        hp, sp = divmod(p, 8)
        pivot = jnp.broadcast_to(cols[p][hp][sp : sp + 1, :], (8, 128))
        scale = lax.rsqrt(pivot)
        line = jnp.broadcast_to(panel[hp][sp : sp + 1, :], (8, 128)) * scale
        done[hp] = jnp.where(sub == sp, line, done[hp])
        scaled = {}
        for h in range(hp, len(rows)):
            if h == hp:
                if sp == 7:
                    continue
                scaled[h] = jnp.where(sub > sp, cols[p][h] * scale, 0.0)
            else:
                scaled[h] = cols[p][h] * scale
        for h, f in scaled.items():
            panel[h] = panel[h] - f * line
        for c in range(p + 1, count):
            hc, sc = divmod(c, 8)
            head = jnp.broadcast_to(scaled[hc][sc : sc + 1, :], (8, 128))
            for h, f in scaled.items():
                if h >= hc:
                    cols[c][h] = cols[c][h] - f * head
    return done


def compress_kernel(panel_id, tiles, places, info, *refs):
    groups = 1 + max(g for g, _ in places.values())
    us, vs = refs[:groups], refs[groups : 2 * groups]
    (top, half, other, lp, uit, sketch, u_out, v_out) = refs[2 * groups : 2 * groups + 8]
    (sk_t, turned, side, side_u, vl_t, nupd, sample, mat, inv) = refs[2 * groups + 8 :]

    def own_u(a, e):
        group, index = places[a, e]
        return us[group][index]

    def own_v(a, e):
        group, index = places[a, e]
        return vs[group][index]

    row_place = info[0]
    col_place = info[1]
    n_row = info[2]
    n_col = info[3]
    lefts = sorted({a for a, _ in tiles})
    tops = sorted({e for _, e in tiles})
    rank_width = sketch.shape[1]
    tile_size = sketch.shape[0]
    root_b = tile_size**0.5
    lane = lax.broadcasted_iota(jnp.int32, (8, 128), 1)
    sub = lax.broadcasted_iota(jnp.int32, (8, 128), 0)
    lane_row = lax.broadcasted_iota(jnp.int32, (1, 128), 1)

    sk_t[...] = sketch[...].T
    for e in tops:
        turned[e] = dot_nn(lp[...], top[e]).astype(BF16)
    first_core = info[10] == 0
    for a in lefts:
        side_u[a] = jnp.where(first_core, half[a], other[a])
        raw_v = jnp.where(first_core, other[a], half[a])
        wide = (dot_nn(uit[...], raw_v) * root_b).astype(BF16)
        side[a] = wide
        vl_t[a] = wide.T
    probe_top = {e: dot_nn(sk_t[...], top[2 + e]) for e in tops}

    def rank_of(a, e):
        return info[4 + a * 2 + e]

    for t, (a, e) in enumerate(tiles):
        coupling = (dot_nn(vl_t[a], turned[e]) * (1.0 / root_b)).astype(BF16)
        product = dot_nn(side_u[a], coupling)
        nupd[t] = (product * (-(rank_width**-0.5))).astype(BF16)
        probe_own = dot_nn(sk_t[...], own_v(a, e))
        high, low = halves(jnp.concatenate([probe_own, probe_top[e]], axis=1))
        both = dot_nt(
            jnp.concatenate([own_u(a, e), nupd[t]], axis=1),
            jnp.concatenate([high, low], axis=0),
        )
        drawn = both[:, :rank_width] + both[:, rank_width:]
        drawn = jnp.where(lane_row < rank_of(a, e), drawn, 0.0)
        high, low = halves(drawn)
        sample[t] = jnp.concatenate([high, low], axis=1)
        gram = dot_tn(sample[t], sample[t])
        w = rank_width
        cross = gram[:w, w:]
        gram = (gram[:w, :w] + gram[w:, w:]) + (cross + gram[w:, :w])
        diag = lax.broadcasted_iota(jnp.int32, (w, w), 0)
        cols = lax.broadcasted_iota(jnp.int32, (w, w), 1)
        mat[t] = gram + jnp.where((diag == cols) & (cols >= rank_of(a, e)), 1.0, 0.0)

    for start in range(0, rank_width, STEP):
        stop = start + STEP
        for t in range(len(tiles)):
            rows = [mat[t, start + 8 * h : start + 8 * h + 8, :] for h in range(STEP // 8)]
            done = factor_block(rows, start, lane, sub)
            for h, piece in enumerate(done):
                inv[t, start + 8 * h : start + 8 * h + 8, :] = jnp.where(
                    lane < stop, piece, 0.0
                )
            if stop < rank_width:
                scaled = jnp.concatenate(done, axis=0)
                h, m, l = thirds(scaled)
                first = jnp.concatenate([h, h, m, m, h, l], axis=0)
                second = jnp.concatenate([h, m, h, m, l, h], axis=0)
                change = dot_nn(first.T[stop:, :], second)
                own = (lane_row >= start) & (lane_row < stop)
                mat[t, stop:, :] = jnp.where(own, 0.0, mat[t, stop:, :]) - change

    for t, (a, e) in enumerate(tiles):
        high, low = halves(inv[t])
        weights = jnp.concatenate(
            [
                jnp.concatenate([high, high], axis=1),
                jnp.concatenate([low, jnp.zeros_like(low)], axis=1),
            ],
            axis=0,
        )
        both = dot_nt(sample[t], weights)
        basis = both[:, :rank_width] + both[:, rank_width:]
        fresh_u = (basis * root_b).astype(BF16)
        high, low = halves(basis)
        left_x = jnp.concatenate([own_u(a, e), nupd[t]], axis=1)
        mixed = dot_tn(jnp.concatenate([high, low], axis=1), left_x)
        high, low = halves(mixed[:rank_width] + mixed[rank_width:])
        both = dot_nt(
            jnp.concatenate([own_v(a, e), top[2 + e]], axis=1),
            jnp.concatenate([high, low], axis=0),
        )
        fresh_v = ((both[:, :rank_width] + both[:, rank_width:]) * (1.0 / root_b)).astype(BF16)
        row_id = a * n_row + row_place
        col_id = e * n_col + col_place
        chosen = (row_id > panel_id) & (col_id > panel_id)
        keep_u = own_u(a, e)
        keep_v = own_v(a, e)
        if a == 0:
            keep_u = jnp.where((row_place == panel_id) & (col_id > panel_id), turned[e], keep_u)
        if e == 0:
            keep_v = jnp.where((col_place == panel_id) & (row_id > panel_id), side[a], keep_v)
        u_out[t] = jnp.where(chosen, fresh_u, keep_u)
        v_out[t] = jnp.where(chosen, fresh_v, keep_v)


def compress(panel_id, tiles, places, info, us, vs, top, half, other, lp, uit, sketch):
    count = len(tiles)
    size, width = sketch.shape
    vmem = pl.BlockSpec(memory_space=pltpu.VMEM)
    shape = jax.ShapeDtypeStruct((count, size, width), BF16)
    flops = 2 * count * size * width * width * 30
    return pl.pallas_call(
        functools.partial(compress_kernel, panel_id, tiles, places),
        out_shape=(shape, shape),
        in_specs=[pl.BlockSpec(memory_space=pltpu.SMEM)] + [vmem] * (2 * len(us) + 6),
        out_specs=(vmem, vmem),
        scratch_shapes=[
            pltpu.VMEM((width, size), BF16),
            pltpu.VMEM((2, size, width), BF16),
            pltpu.VMEM((3, size, width), BF16),
            pltpu.VMEM((3, size, width), BF16),
            pltpu.VMEM((3, width, size), BF16),
            pltpu.VMEM((count, size, width), BF16),
            pltpu.VMEM((count, size, 2 * width), BF16),
            pltpu.VMEM((count, width, width), F32),
            pltpu.VMEM((count, width, width), F32),
        ],
        cost_estimate=pl.CostEstimate(
            flops=flops, bytes_accessed=8 * count * size * width, transcendentals=0
        ),
    )(info, *us, *vs, top, half, other, lp, uit, sketch)


ROW = ("y", "z")
COL = ("x", "core")


def spread_row(pieces, root):
    n_y, n_z = lax.axis_size("y"), lax.axis_size("z")
    y, z = lax.axis_index("y"), lax.axis_index("z")
    part = jnp.where((y == 0) & (z == root), pieces[0], 0)
    for k in range(1, n_y):
        part = part + lax.ppermute(pieces[k], ROW, [(root, k * n_z + root)])
    held = [root]
    stride = n_z // 2
    while stride:
        fresh = [(place + stride) % n_z for place in held]
        pairs = [
            (k * n_z + a, k * n_z + b) for k in range(n_y) for a, b in zip(held, fresh)
        ]
        part = part + lax.ppermute(part, ROW, pairs)
        held = held + fresh
        stride //= 2
    return lax.all_gather(part, "y")


def spread_col(side_u, side_v, root):
    n_core = lax.axis_size("core")
    x, core = lax.axis_index("x"), lax.axis_index("core")
    here_u, here_v = (
        lax.ppermute(side, COL, [(root, n_core - 1 - root)]) for side in (side_u, side_v)
    )
    sent = here_v if root == 0 else here_u
    kept = side_u if root == 0 else side_v
    half = jnp.where(core == root, kept, sent)
    start = jnp.where(x == 0, half, 0)
    half = start + lax.ppermute(start, "x", [(0, 1)]) + lax.ppermute(start, "x", [(0, 3)])
    cut = half.shape[1] // 2
    low = lax.ppermute(half[:, :cut], "x", [(1, 2)])
    high = lax.ppermute(half[:, cut:], "x", [(3, 2)])
    half = half + jnp.concatenate([low, high], axis=1)
    other = lax.ppermute(half, "core", [(0, 1), (1, 0)])
    return half, other


ALL = ((0, 0), (0, 1), (1, 0), (1, 1), (2, 0), (2, 1))
HEAD = ((0, 0), (0, 1), (1, 0), (2, 0))
INNER = ((1, 1), (2, 1))


def on_device(tile_u, tile_v, tile_ranks, lower_inverse, upper_inverse, row_order, sketch):
    size, width = sketch.shape
    count = len(ALL)
    ranks = tile_ranks.reshape(count)
    keep = (jnp.arange(width, dtype=jnp.int32)[None, :] < ranks[:, None])[:, None, :]
    u = jnp.where(keep, tile_u.reshape(count, size, width), 0)
    v = jnp.where(keep, tile_v.reshape(count, size, width), 0)
    places = jnp.stack(
        [
            lax.axis_index(ROW),
            lax.axis_index(COL),
            jnp.int32(lax.axis_size(ROW)),
            jnp.int32(lax.axis_size(COL)),
        ]
    ).astype(jnp.int32)
    info = jnp.concatenate([places, ranks, lax.axis_index("core").reshape(1).astype(jnp.int32)])
    spots = jnp.arange(size, dtype=jnp.int32)
    pick = (row_order[:, :, None] == spots[None, None, :]).astype(BF16)
    lower = jnp.einsum("kap,kpb->kab", lower_inverse, pick, preferred_element_type=F32).astype(BF16)
    upper = jnp.swapaxes(upper_inverse, 1, 2)

    top = spread_row((u[0], u[1], v[0], v[1]), 0)
    half, other = spread_col(u[0::2], v[0::2], 0)
    flat = {tile: (0, n) for n, tile in enumerate(ALL)}
    shared = (top, half, other, lower[0], upper[0], sketch)
    head_u, head_v = compress(0, HEAD, flat, info, (u,), (v,), *shared)
    top = spread_row((head_u[0], head_u[1], head_v[0], head_v[1]), 1)
    side_u = jnp.concatenate([head_u[:1], head_u[2:]])
    side_v = jnp.concatenate([head_v[:1], head_v[2:]])
    half, other = spread_col(side_u, side_v, 1)
    inner_u, inner_v = compress(0, INNER, flat, info, (u,), (v,), *shared)
    split = {tile: (0, n) for n, tile in enumerate(HEAD)}
    split.update({tile: (1, n) for n, tile in enumerate(INNER)})
    shared = (top, half, other, lower[1], upper[1], sketch)
    u, v = compress(1, ALL, split, info, (head_u, inner_u), (head_v, inner_v), *shared)
    return u.reshape(tile_u.shape), v.reshape(tile_v.shape)


def solution(mesh):
    split = Mesh(mesh.devices.reshape(4, 8, 4, 2), ("y", "z", "x", "core"))
    tiles = P(None, ROW, None, COL, None, None)
    return jax.shard_map(
        on_device,
        mesh=split,
        in_specs=(tiles, tiles, P(None, ROW, None, COL), P(), P(), P(), P()),
        out_specs=(tiles, tiles),
        check_vma=False,
    )
```

```python
import functools

import jax
import jax.numpy as jnp
from jax import lax
from jax.experimental import pallas as pl
from jax.experimental.pallas import tpu as pltpu
from jax.sharding import Mesh
from jax.sharding import PartitionSpec as P

PANELS = 2
STEP = 16
F32 = jnp.float32
BF16 = jnp.bfloat16


def dot_nn(a, b):
    return lax.dot_general(a, b, (((1,), (0,)), ((), ())), preferred_element_type=F32)


def dot_nt(a, b):
    return lax.dot_general(a, b, (((1,), (1,)), ((), ())), preferred_element_type=F32)


def dot_tn(a, b):
    return lax.dot_general(a, b, (((0,), (0,)), ((), ())), preferred_element_type=F32)


def halves(x):
    high = x.astype(BF16)
    return high, (x - high.astype(F32)).astype(BF16)


def thirds(x):
    high = x.astype(BF16)
    rest = x - high.astype(F32)
    middle = rest.astype(BF16)
    return high, middle, (rest - middle.astype(F32)).astype(BF16)


def factor_block(rows, start, lane, sub):
    count = len(rows) * 8
    cols = [
        [
            jnp.broadcast_to(rows[h][:, start + c : start + c + 1], (8, 128))
            if c < 8 * (h + 1)
            else None
            for h in range(len(rows))
        ]
        for c in range(count)
    ]
    panel = []
    for h in range(len(rows)):
        own = (lane >= start) & (lane < start + count)
        unit = (lane == sub + (start + 8 * h)).astype(F32)
        panel.append(jnp.where(own, unit, rows[h]))
    done = [jnp.zeros((8, 128), F32) for _ in rows]
    for p in range(count):
        hp, sp = divmod(p, 8)
        pivot = jnp.broadcast_to(cols[p][hp][sp : sp + 1, :], (8, 128))
        scale = lax.rsqrt(pivot)
        line = jnp.broadcast_to(panel[hp][sp : sp + 1, :], (8, 128)) * scale
        done[hp] = jnp.where(sub == sp, line, done[hp])
        scaled = {}
        for h in range(hp, len(rows)):
            if h == hp:
                if sp == 7:
                    continue
                scaled[h] = jnp.where(sub > sp, cols[p][h] * scale, 0.0)
            else:
                scaled[h] = cols[p][h] * scale
        for h, f in scaled.items():
            panel[h] = panel[h] - f * line
        for c in range(p + 1, count):
            hc, sc = divmod(c, 8)
            head = jnp.broadcast_to(scaled[hc][sc : sc + 1, :], (8, 128))
            for h, f in scaled.items():
                if h >= hc:
                    cols[c][h] = cols[c][h] - f * head
    return done


def compress_kernel(panel_id, tiles, places, sends, grid, info, *refs):
    groups = 1 + max(g for g, _ in places.values())
    us, vs = refs[:groups], refs[groups : 2 * groups]
    parts = refs[2 * groups : 2 * groups + 4]
    (half, other, lp, uit, sketch) = refs[2 * groups + 4 : 2 * groups + 9]
    outs = refs[2 * groups + 9 : len(refs) - 10]
    (top, sk_t, turned, side, side_u, vl_t, nupd, sample, mat, inv) = refs[len(refs) - 10 :]
    row_place = info[0]
    col_place = info[1]
    n_row, n_col = grid
    first_core = info[8] == 0
    y = info[9]
    lefts = sorted({a for a, _ in tiles})
    tops = sorted({e for _, e in tiles})
    rank_width = sketch.shape[1]
    tile_size = sketch.shape[0]
    root_b = tile_size**0.5
    lane = lax.broadcasted_iota(jnp.int32, (8, 128), 1)
    sub = lax.broadcasted_iota(jnp.int32, (8, 128), 0)
    lane_row = lax.broadcasted_iota(jnp.int32, (1, 128), 1)

    def rank_of(a, e):
        return info[2 + a * 2 + e]

    def load(which, a, e):
        group, index = places[a, e]
        value = which[group][index]
        if panel_id == 0:
            value = value * (lane_row < rank_of(a, e)).astype(F32).astype(BF16)
        return value

    for k in range(4):
        turn = (k - y + 4) % 4
        near = jnp.where(turn == 0, parts[0][...], parts[1][...])
        far = jnp.where(turn == 2, parts[2][...], parts[3][...])
        if k % 2 in tops:
            top[k] = jnp.where(turn < 2, near, far)
    sk_t[...] = sketch[...].T
    for e in tops:
        turned[e] = dot_nn(lp[...], top[e]).astype(BF16)
    for a in lefts:
        side_u[a] = jnp.where(first_core, half[a], other[a])
        raw_v = jnp.where(first_core, other[a], half[a])
        wide = (dot_nn(uit[...], raw_v) * root_b).astype(BF16)
        side[a] = wide
        vl_t[a] = wide.T
    probe_top = {e: dot_nn(sk_t[...], top[2 + e]) for e in tops}

    for t, (a, e) in enumerate(tiles):
        coupling = (dot_nn(vl_t[a], turned[e]) * (1.0 / root_b)).astype(BF16)
        product = dot_nn(side_u[a], coupling)
        nupd[t] = (product * (-(rank_width**-0.5))).astype(BF16)
        probe_own = dot_nn(sk_t[...], load(vs, a, e))
        high, low = halves(jnp.concatenate([probe_own, probe_top[e]], axis=1))
        both = dot_nt(
            jnp.concatenate([load(us, a, e), nupd[t]], axis=1),
            jnp.concatenate([high, low], axis=0),
        )
        drawn = both[:, :rank_width] + both[:, rank_width:]
        drawn = jnp.where(lane_row < rank_of(a, e), drawn, 0.0)
        high, low = halves(drawn)
        sample[t] = jnp.concatenate([high, low], axis=1)
        gram = dot_tn(sample[t], sample[t])
        w = rank_width
        cross = gram[:w, w:]
        gram = (gram[:w, :w] + gram[w:, w:]) + (cross + gram[w:, :w])
        diag = lax.broadcasted_iota(jnp.int32, (w, w), 0)
        cols = lax.broadcasted_iota(jnp.int32, (w, w), 1)
        mat[t] = gram + jnp.where((diag == cols) & (cols >= rank_of(a, e)), 1.0, 0.0)

    for start in range(0, rank_width, STEP):
        stop = start + STEP
        for t in range(len(tiles)):
            rows = [mat[t, start + 8 * h : start + 8 * h + 8, :] for h in range(STEP // 8)]
            done = factor_block(rows, start, lane, sub)
            for h, piece in enumerate(done):
                inv[t, start + 8 * h : start + 8 * h + 8, :] = jnp.where(
                    lane < stop, piece, 0.0
                )
            if stop < rank_width:
                scaled = jnp.concatenate(done, axis=0)
                h, m, l = thirds(scaled)
                first = jnp.concatenate([h, h, m, m, h, l], axis=0)
                second = jnp.concatenate([h, m, h, m, l, h], axis=0)
                change = dot_nn(first.T[stop:, :], second)
                own = (lane_row >= start) & (lane_row < stop)
                mat[t, stop:, :] = jnp.where(own, 0.0, mat[t, stop:, :]) - change

    for t, (a, e) in enumerate(tiles):
        high, low = halves(inv[t])
        weights = jnp.concatenate(
            [
                jnp.concatenate([high, high], axis=1),
                jnp.concatenate([low, jnp.zeros_like(low)], axis=1),
            ],
            axis=0,
        )
        both = dot_nt(sample[t], weights)
        basis = both[:, :rank_width] + both[:, rank_width:]
        fresh_u = (basis * root_b).astype(BF16)
        keep_u = load(us, a, e)
        keep_v = load(vs, a, e)
        mixed = dot_tn(fresh_u, jnp.concatenate([keep_u, nupd[t]], axis=1))
        own_right = jnp.concatenate([keep_v, top[2 + e]], axis=1)
        if panel_id == PANELS - 1:
            right = dot_nt(own_right, mixed.astype(BF16))
        else:
            both = dot_nt(own_right, jnp.concatenate(halves(mixed), axis=0))
            right = both[:, :rank_width] + both[:, rank_width:]
        fresh_v = (right * (1.0 / tile_size)).astype(BF16)
        row_id = a * n_row + row_place
        col_id = e * n_col + col_place
        chosen = (row_id > panel_id) & (col_id > panel_id)
        settled = a * n_row > panel_id and e * n_col > panel_id
        if a == 0:
            keep_u = jnp.where((row_place == panel_id) & (col_id > panel_id), turned[e], keep_u)
        if e == 0:
            keep_v = jnp.where((col_place == panel_id) & (row_id > panel_id), side[a], keep_v)
        new_u = fresh_u if settled else jnp.where(chosen, fresh_u, keep_u)
        new_v = fresh_v if settled else jnp.where(chosen, fresh_v, keep_v)
        for out, index in sends[a, e][0]:
            outs[out][index] = new_u
        for out, index in sends[a, e][1]:
            outs[out][index] = new_v


def compress(panel_id, tiles, places, sends, depths, info, us, vs, parts, *shared):
    count = len(tiles)
    size, width = shared[-1].shape
    vmem = pl.BlockSpec(memory_space=pltpu.VMEM)
    grid = (lax.axis_size(ROW), lax.axis_size(COL))
    flops = 2 * count * size * width * width * 30
    return pl.pallas_call(
        functools.partial(compress_kernel, panel_id, tiles, places, sends, grid),
        out_shape=[
            jax.ShapeDtypeStruct((depth,) * (depth > 0) + (size, width), BF16) for depth in depths
        ],
        in_specs=[pl.BlockSpec(memory_space=pltpu.SMEM)] + [vmem] * (2 * len(us) + 9),
        out_specs=[vmem] * len(depths),
        scratch_shapes=[
            pltpu.VMEM((4, size, width), BF16),
            pltpu.VMEM((width, size), BF16),
            pltpu.VMEM((2, size, width), BF16),
            pltpu.VMEM((3, size, width), BF16),
            pltpu.VMEM((3, size, width), BF16),
            pltpu.VMEM((3, width, size), BF16),
            pltpu.VMEM((count, size, width), BF16),
            pltpu.VMEM((count, size, 2 * width), BF16),
            pltpu.VMEM((count, width, width), F32),
            pltpu.VMEM((count, width, width), F32),
        ],
        compiler_params=pltpu.CompilerParams(vmem_limit_bytes=24 * 2**20),
        cost_estimate=pl.CostEstimate(
            flops=flops, bytes_accessed=8 * count * size * width, transcendentals=0
        ),
    )(info, *us, *vs, *parts, *shared)


ROW = ("y", "z")
COL = ("x", "core")


def spread_row(pieces, root):
    n_y, n_z = lax.axis_size("y"), lax.axis_size("z")
    y, z = lax.axis_index("y"), lax.axis_index("z")
    part = jnp.where((y == 0) & (z == root), pieces[0], 0)
    for k in range(1, n_y):
        part = part + lax.ppermute(pieces[k], ROW, [(root, k * n_z + root)])

    def along_z(hops):
        pairs = [
            (k * n_z + (root + a) % n_z, k * n_z + (root + b) % n_z)
            for k in range(n_y)
            for a, b in hops
        ]
        return lax.ppermute(part, ROW, pairs)

    part = part + along_z([(0, 3)]) + along_z([(0, 5)])
    part = part + along_z([(0, 1), (3, 4), (5, 6)]) + along_z([(0, 7), (3, 2)])
    return [part] + [
        lax.ppermute(part, "y", [((k + s) % n_y, k) for k in range(n_y)]) for s in range(1, n_y)
    ]


def spread_col(side_u, side_v, root):
    n_core = lax.axis_size("core")
    x, core = lax.axis_index("x"), lax.axis_index("core")
    kept, given = (side_u, side_v) if root == 0 else (side_v, side_u)
    sent = lax.ppermute(given, COL, [(root, n_core - 1 - root)])
    start = jnp.where(x == 0, jnp.where(core == root, kept, sent), 0)
    half = start + lax.ppermute(start, "x", [(0, 1)]) + lax.ppermute(start, "x", [(0, 3)])
    cut = half.shape[1] // 2
    low = lax.ppermute(half[:, :cut], "x", [(1, 2)])
    high = lax.ppermute(half[:, cut:], "x", [(3, 2)])
    half = half + jnp.concatenate([low, high], axis=1)
    other = lax.ppermute(half, "core", [(0, 1), (1, 0)])
    return half, other


ALL = ((0, 0), (0, 1), (1, 0), (1, 1), (2, 0), (2, 1))
HEAD = ((0, 0), (0, 1), (1, 0), (2, 0))
INNER = ((1, 1), (2, 1))
WHOLE = Ellipsis


def on_device(tile_u, tile_v, tile_ranks, lower_inverse, upper_inverse, row_order, sketch):
    size, width = sketch.shape
    count = len(ALL)
    ranks = tile_ranks.reshape(count)
    keep = (jnp.arange(width, dtype=jnp.int32)[None, :] < ranks[:, None])[:, None, :]
    u = tile_u.reshape(count, size, width)
    v = tile_v.reshape(count, size, width)
    places = jnp.stack([lax.axis_index(ROW), lax.axis_index(COL)]).astype(jnp.int32)
    last = jnp.stack([lax.axis_index("core"), lax.axis_index("y")]).astype(jnp.int32)
    info = jnp.concatenate([places, ranks, last])
    spots = jnp.arange(size, dtype=jnp.int32)
    pick = (row_order[:, :, None] == spots[None, None, :]).astype(BF16)
    lower = jnp.einsum("kap,kpb->kab", lower_inverse, pick, preferred_element_type=F32).astype(BF16)
    upper = jnp.swapaxes(upper_inverse, 1, 2)

    pieces = [jnp.where(keep[n], x[n], 0) for x in (u, v) for n in (0, 1)]
    parts = spread_row(pieces, 0)
    half, other = spread_col(
        jnp.where(keep[0::2], u[0::2], 0), jnp.where(keep[0::2], v[0::2], 0), 0
    )
    flat = {tile: (0, n) for n, tile in enumerate(ALL)}
    shared = (parts, half, other, lower[0], upper[0], sketch)
    sends = {
        (0, 0): ([(0, WHOLE), (4, 0)], [(2, WHOLE), (5, 0)]),
        (0, 1): ([(1, WHOLE)], [(3, WHOLE)]),
        (1, 0): ([(4, 1)], [(5, 1)]),
        (2, 0): ([(4, 2)], [(5, 2)]),
    }
    *pieces, side_u, side_v = compress(
        0, HEAD, flat, sends, (0, 0, 0, 0, 3, 3), info, (u,), (v,), *shared
    )
    parts = spread_row(pieces, 1)
    half, other = spread_col(side_u, side_v, 1)
    sends = {tile: ([(0, n)], [(1, n)]) for n, tile in enumerate(INNER)}
    inner_u, inner_v = compress(0, INNER, flat, sends, (2, 2), info, (u,), (v,), *shared)
    split = {
        (0, 0): (0, 0),
        (1, 0): (0, 1),
        (2, 0): (0, 2),
        (0, 1): (1, WHOLE),
        (1, 1): (2, 0),
        (2, 1): (2, 1),
    }
    sends = {tile: ([(0, n)], [(1, n)]) for n, tile in enumerate(ALL)}
    shared = (parts, half, other, lower[1], upper[1], sketch)
    u, v = compress(
        1,
        ALL,
        split,
        sends,
        (count, count),
        info,
        (side_u, pieces[1], inner_u),
        (side_v, pieces[3], inner_v),
        *shared,
    )
    return u.reshape(tile_u.shape), v.reshape(tile_v.shape)


def solution(mesh):
    split = Mesh(mesh.devices.reshape(4, 8, 4, 2), ("y", "z", "x", "core"))
    tiles = P(None, ROW, None, COL, None, None)
    return jax.shard_map(
        on_device,
        mesh=split,
        in_specs=(tiles, tiles, P(None, ROW, None, COL), P(), P(), P(), P()),
        out_specs=(tiles, tiles),
        check_vma=False,
    )
```

```python
import functools

import jax
import jax.numpy as jnp
from jax import lax
from jax.experimental import pallas as pl
from jax.experimental.pallas import tpu as pltpu
from jax.sharding import Mesh
from jax.sharding import PartitionSpec as P


PANELS = 2
STEP = 16
F32 = jnp.float32
BF16 = jnp.bfloat16


def dot_nn(a, b):
    return lax.dot_general(a, b, (((1,), (0,)), ((), ())), preferred_element_type=F32)


def dot_nt(a, b):
    return lax.dot_general(a, b, (((1,), (1,)), ((), ())), preferred_element_type=F32)


def dot_tn(a, b):
    return lax.dot_general(a, b, (((0,), (0,)), ((), ())), preferred_element_type=F32)


def halves(x):
    high = x.astype(BF16)
    return high, (x - high.astype(F32)).astype(BF16)


def thirds(x):
    high = x.astype(BF16)
    rest = x - high.astype(F32)
    middle = rest.astype(BF16)
    return high, middle, (rest - middle.astype(F32)).astype(BF16)


def factor_block(rows, blocks, start, lane, sub):
    count = len(rows) * 8
    cols = [
        [
            jnp.broadcast_to(blocks[h][:, c : c + 1], (8, 128))
            if c < 8 * (h + 1)
            else None
            for h in range(len(rows))
        ]
        for c in range(count)
    ]
    panel = []
    for h in range(len(rows)):
        own = (lane >= start) & (lane < start + count)
        unit = (lane == sub + (start + 8 * h)).astype(F32)
        panel.append(jnp.where(own, unit, rows[h]))
    done = [jnp.zeros((8, 128), F32) for _ in rows]
    for p in range(count):
        hp, sp = divmod(p, 8)
        pivot = jnp.broadcast_to(cols[p][hp][sp : sp + 1, :], (8, 128))
        scale = lax.rsqrt(pivot)
        line = jnp.broadcast_to(panel[hp][sp : sp + 1, :], (8, 128)) * scale
        done[hp] = jnp.where(sub == sp, line, done[hp])
        scaled = {}
        for h in range(hp, len(rows)):
            if h == hp:
                if sp == 7:
                    continue
                scaled[h] = jnp.where(sub > sp, cols[p][h] * scale, 0.0)
            else:
                scaled[h] = cols[p][h] * scale
        for h, f in scaled.items():
            panel[h] = panel[h] - f * line
        for c in range(p + 1, count):
            hc, sc = divmod(c, 8)
            head = jnp.broadcast_to(scaled[hc][sc : sc + 1, :], (8, 128))
            for h, f in scaled.items():
                if h >= hc:
                    cols[c][h] = cols[c][h] - f * head
    return done


def compress_kernel(panel_id, tiles, places, sends, grid, info, *refs):
    groups = 1 + max(g for g, _ in places.values())
    us, vs = refs[:groups], refs[groups : 2 * groups]
    parts = refs[2 * groups : 2 * groups + 4]
    (half, other, lp, upper, sketch) = refs[2 * groups + 4 : 2 * groups + 9]
    outs = refs[2 * groups + 9 : len(refs) - 10]
    (top, sk_t, turned, side, side_u, vl_t, nupd, sample, mat, inv) = refs[len(refs) - 10 :]
    row_place = info[0]
    col_place = info[1]
    n_row, n_col = grid
    first_core = info[8] == 0
    y = info[9]
    lefts = sorted({a for a, _ in tiles})
    tops = sorted({e for _, e in tiles})
    rank_width = sketch.shape[1]
    tile_size = sketch.shape[0]
    root_b = tile_size**0.5
    lane = lax.broadcasted_iota(jnp.int32, (8, 128), 1)
    sub = lax.broadcasted_iota(jnp.int32, (8, 128), 0)
    lane_row = lax.broadcasted_iota(jnp.int32, (1, 128), 1)

    def rank_of(a, e):
        return info[2 + a * 2 + e]

    def load(which, a, e):
        group, index = places[a, e]
        value = which[group][index]
        if panel_id == 0:
            value = value * (lane_row < rank_of(a, e)).astype(F32).astype(BF16)
        return value

    for k in range(4):
        turn = (k - y + 4) % 4
        near = jnp.where(turn == 0, parts[0][...], parts[1][...])
        far = jnp.where(turn == 2, parts[2][...], parts[3][...])
        if k % 2 in tops:
            top[k] = jnp.where(turn < 2, near, far)
    sk_t[...] = sketch[...].T
    for e in tops:
        turned[e] = dot_nn(lp[panel_id], top[e]).astype(BF16)
    upper_t = upper[panel_id].T
    for a in lefts:
        side_u[a] = jnp.where(first_core, half[a], other[a])
        raw_v = jnp.where(first_core, other[a], half[a])
        wide = (dot_nn(upper_t, raw_v) * root_b).astype(BF16)
        side[a] = wide
        vl_t[a] = wide.T
    probe_top = {e: dot_nn(sk_t[...], top[2 + e]) for e in tops}

    for t, (a, e) in enumerate(tiles):
        coupling = (dot_nn(vl_t[a], turned[e]) * (1.0 / root_b)).astype(BF16)
        product = dot_nn(side_u[a], coupling)
        nupd[t] = (product * (-(rank_width**-0.5))).astype(BF16)
        probe_own = dot_nn(sk_t[...], load(vs, a, e))
        high, low = halves(jnp.concatenate([probe_own, probe_top[e]], axis=1))
        both = dot_nt(
            jnp.concatenate([load(us, a, e), nupd[t]], axis=1),
            jnp.concatenate([high, low], axis=0),
        )
        drawn = both[:, :rank_width] + both[:, rank_width:]
        drawn = jnp.where(lane_row < rank_of(a, e), drawn, 0.0)
        high, low = halves(drawn)
        sample[t] = jnp.concatenate([high, low], axis=1)
        gram = dot_tn(sample[t], sample[t])
        w = rank_width
        cross = gram[:w, w:]
        gram = (gram[:w, :w] + gram[w:, w:]) + (cross + gram[w:, :w])
        diag = lax.broadcasted_iota(jnp.int32, (w, w), 0)
        cols = lax.broadcasted_iota(jnp.int32, (w, w), 1)
        mat[t] = gram + jnp.where((diag == cols) & (cols >= rank_of(a, e)), 1.0, 0.0)

    def update(scaled):
        h, m, l = thirds(scaled)
        first = jnp.concatenate([h, h, m, m, h, l], axis=0)
        return first.T, jnp.concatenate([h, m, h, m, l, h], axis=0)

    for start in range(0, rank_width, STEP):
        stop = start + STEP
        for t in range(len(tiles)):
            rows = [mat[t, start + 8 * h : start + 8 * h + 8, :] for h in range(STEP // 8)]
            blocks = [row[:, start:stop] for row in rows]
            done = factor_block(rows, blocks, start, lane, sub)
            for h, piece in enumerate(done):
                inv[t, start + 8 * h : start + 8 * h + 8, :] = jnp.where(
                    lane < stop, piece, 0.0
                )
            if stop < rank_width:
                first, second = update(jnp.concatenate(done, axis=0))
                change = dot_nn(first[stop:, :], second)
                own = (lane_row >= start) & (lane_row < stop)
                mat[t, stop:, :] = jnp.where(own, 0.0, mat[t, stop:, :]) - change

    for t, (a, e) in enumerate(tiles):
        high, low = halves(inv[t])
        weights = jnp.concatenate(
            [
                jnp.concatenate([high, high], axis=1),
                jnp.concatenate([low, jnp.zeros_like(low)], axis=1),
            ],
            axis=0,
        )
        both = dot_nt(sample[t], weights)
        basis = both[:, :rank_width] + both[:, rank_width:]
        fresh_u = (basis * root_b).astype(BF16)
        keep_u = load(us, a, e)
        keep_v = load(vs, a, e)
        mixed = dot_tn(fresh_u, jnp.concatenate([keep_u, nupd[t]], axis=1))
        own_right = jnp.concatenate([keep_v, top[2 + e]], axis=1)
        if panel_id == PANELS - 1:
            right = dot_nt(own_right, mixed.astype(BF16))
        else:
            both = dot_nt(own_right, jnp.concatenate(halves(mixed), axis=0))
            right = both[:, :rank_width] + both[:, rank_width:]
        fresh_v = (right * (1.0 / tile_size)).astype(BF16)
        row_id = a * n_row + row_place
        col_id = e * n_col + col_place
        chosen = (row_id > panel_id) & (col_id > panel_id)
        settled = a * n_row > panel_id and e * n_col > panel_id
        if a == 0:
            keep_u = jnp.where((row_place == panel_id) & (col_id > panel_id), turned[e], keep_u)
        if e == 0:
            keep_v = jnp.where((col_place == panel_id) & (row_id > panel_id), side[a], keep_v)
        new_u = fresh_u if settled else jnp.where(chosen, fresh_u, keep_u)
        new_v = fresh_v if settled else jnp.where(chosen, fresh_v, keep_v)
        for out, index in sends[a, e][0]:
            outs[out][index] = new_u
        for out, index in sends[a, e][1]:
            outs[out][index] = new_v


def compress(
    panel_id, tiles, places, sends, depths, info, us, vs, parts, *shared
):
    count = len(tiles)
    size, width = shared[-1].shape
    vmem = pl.BlockSpec(memory_space=pltpu.VMEM)
    grid = (lax.axis_size(ROW), lax.axis_size(COL))
    flops = 2 * count * size * width * width * 30
    return pl.pallas_call(
        functools.partial(compress_kernel, panel_id, tiles, places, sends, grid),
        out_shape=[
            jax.ShapeDtypeStruct((depth,) * (depth > 0) + (size, width), BF16) for depth in depths
        ],
        in_specs=[pl.BlockSpec(memory_space=pltpu.SMEM)] + [vmem] * (2 * len(us) + 9),
        out_specs=[vmem] * len(depths),
        scratch_shapes=[
            pltpu.VMEM((4, size, width), BF16),
            pltpu.VMEM((width, size), BF16),
            pltpu.VMEM((2, size, width), BF16),
            pltpu.VMEM((3, size, width), BF16),
            pltpu.VMEM((3, size, width), BF16),
            pltpu.VMEM((3, width, size), BF16),
            pltpu.VMEM((count, size, width), BF16),
            pltpu.VMEM((count, size, 2 * width), BF16),
            pltpu.VMEM((count, width, width), F32),
            pltpu.VMEM((count, width, width), F32),
        ],
        compiler_params=pltpu.CompilerParams(vmem_limit_bytes=10 * 2**20),
        cost_estimate=pl.CostEstimate(
            flops=flops, bytes_accessed=8 * count * size * width, transcendentals=0
        ),
    )(info, *us, *vs, *parts, *shared)


ROW = ("y", "z")
COL = ("x", "core")


def spread_row(pieces, root):
    n_y, n_z = lax.axis_size("y"), lax.axis_size("z")
    y, z = lax.axis_index("y"), lax.axis_index("z")
    part = jnp.where((y == 0) & (z == root), pieces[0], 0)
    sent = [lax.ppermute(pieces[k], ROW, [(root, k * n_z + root)]) for k in range(1, n_y)]
    part = part + sent[0] + sent[1] + sent[2]

    def along_z(hops):
        pairs = [
            (k * n_z + (root + a) % n_z, k * n_z + (root + b) % n_z)
            for k in range(n_y)
            for a, b in hops
        ]
        return lax.ppermute(part, ROW, pairs)

    sent = [along_z([(0, 3)]), along_z([(0, 5)])]
    part = part + sent[0] + sent[1]
    sent = [along_z([(0, 1), (3, 4), (5, 6)]), along_z([(0, 7), (3, 2)])]
    part = part + sent[0] + sent[1]
    sent = [lax.ppermute(part, "y", [((k + s) % n_y, k) for k in range(n_y)]) for s in (2, 1, 3)]
    return [part, sent[1], sent[0], sent[2]]


def spread_col(side_u, side_v, root):
    n_core = lax.axis_size("core")
    x, core = lax.axis_index("x"), lax.axis_index("core")
    kept, given = (side_u, side_v) if root == 0 else (side_v, side_u)
    sent = lax.ppermute(given, COL, [(root, n_core - 1 - root)])
    start = jnp.where(x == 0, jnp.where(core == root, kept, sent), 0)
    sent = [lax.ppermute(start, "x", [(0, 1)]), lax.ppermute(start, "x", [(0, 3)])]
    half = start + sent[0] + sent[1]
    cut = half.shape[1] // 2
    low = lax.ppermute(half[:, :cut], "x", [(1, 2)])
    high = lax.ppermute(half[:, cut:], "x", [(3, 2)])
    half = half + jnp.concatenate([low, high], axis=1)
    other = lax.ppermute(half, "core", [(0, 1), (1, 0)])
    return half, other


ALL = ((0, 0), (0, 1), (1, 0), (1, 1), (2, 0), (2, 1))
HEAD = ((0, 0), (0, 1), (1, 0), (2, 0))
INNER = ((1, 1), (2, 1))
WHOLE = Ellipsis


def on_device(tile_u, tile_v, tile_ranks, lower_inverse, upper_inverse, row_order, sketch):
    size, width = sketch.shape
    count = len(ALL)
    ranks = tile_ranks.reshape(count)
    keep = (jnp.arange(width, dtype=jnp.int32)[None, :] < ranks[:, None])[:, None, :]
    u = tile_u.reshape(count, size, width)
    v = tile_v.reshape(count, size, width)
    places = jnp.stack([lax.axis_index(ROW), lax.axis_index(COL)]).astype(jnp.int32)
    last = jnp.stack([lax.axis_index("core"), lax.axis_index("y")]).astype(jnp.int32)
    info = jnp.concatenate([places, ranks, last])
    spots = jnp.arange(size, dtype=jnp.int32)

    pieces = [jnp.where(keep[n], x[n], 0) for x in (u, v) for n in (0, 1)]
    parts = spread_row(pieces, 0)
    half, other = spread_col(
        jnp.where(keep[0::2], u[0::2], 0), jnp.where(keep[0::2], v[0::2], 0), 0
    )
    flat = {tile: (0, n) for n, tile in enumerate(ALL)}
    pick = (row_order[:, :, None] == spots[None, None, :]).astype(BF16)
    lower = jnp.einsum("kap,kpb->kab", lower_inverse, pick, preferred_element_type=F32).astype(BF16)
    shared = (parts, half, other, lower, upper_inverse, sketch)
    sends = {
        (0, 0): ([(0, WHOLE), (4, 0)], [(2, WHOLE), (5, 0)]),
        (0, 1): ([(1, WHOLE)], [(3, WHOLE)]),
        (1, 0): ([(4, 1)], [(5, 1)]),
        (2, 0): ([(4, 2)], [(5, 2)]),
    }
    *pieces, side_u, side_v = compress(
        0, HEAD, flat, sends, (0, 0, 0, 0, 3, 3), info, (u,), (v,), *shared
    )
    parts = spread_row(pieces, 1)
    half, other = spread_col(side_u, side_v, 1)
    sends = {tile: ([(0, n)], [(1, n)]) for n, tile in enumerate(INNER)}
    inner_u, inner_v = compress(
        0, INNER, flat, sends, (2, 2), info, (u,), (v,), *shared
    )
    split = {
        (0, 0): (0, 0),
        (1, 0): (0, 1),
        (2, 0): (0, 2),
        (0, 1): (1, WHOLE),
        (1, 1): (2, 0),
        (2, 1): (2, 1),
    }
    sends = {tile: ([(0, n)], [(1, n)]) for n, tile in enumerate(ALL)}
    shared = (parts, half, other, lower, upper_inverse, sketch)
    ours = ((side_u, pieces[1], inner_u), (side_v, pieces[3], inner_v))
    u, v = compress(1, ALL, split, sends, (count, count), info, *ours, *shared)
    return u.reshape(tile_u.shape), v.reshape(tile_v.shape)


def solution(mesh):
    split = Mesh(mesh.devices.reshape(4, 8, 4, 2), ("y", "z", "x", "core"))
    tiles = P(None, ROW, None, COL, None, None)
    return jax.shard_map(
        on_device,
        mesh=split,
        in_specs=(tiles, tiles, P(None, ROW, None, COL), P(), P(), P(), P()),
        out_specs=(tiles, tiles),
        check_vma=False,
    )
```

```python
import functools

import jax
import jax.numpy as jnp
from jax import lax
from jax.experimental import pallas as pl
from jax.experimental.pallas import tpu as pltpu
from jax.sharding import Mesh
from jax.sharding import PartitionSpec as P


PANELS = 2
STEP = 16
F32 = jnp.float32
BF16 = jnp.bfloat16


def dot_nn(a, b):
    return lax.dot_general(a, b, (((1,), (0,)), ((), ())), preferred_element_type=F32)


def dot_nt(a, b):
    return lax.dot_general(a, b, (((1,), (1,)), ((), ())), preferred_element_type=F32)


def dot_tn(a, b):
    return lax.dot_general(a, b, (((0,), (0,)), ((), ())), preferred_element_type=F32)


def halves(x):
    high = x.astype(BF16)
    return high, (x - high.astype(F32)).astype(BF16)


def thirds(x):
    high = x.astype(BF16)
    rest = x - high.astype(F32)
    middle = rest.astype(BF16)
    return high, middle, (rest - middle.astype(F32)).astype(BF16)


def factor_block(rows, blocks, start, lane, sub):
    count = len(rows) * 8
    cols = [
        [
            jnp.broadcast_to(blocks[h][:, c : c + 1], (8, 128))
            if c < 8 * (h + 1)
            else None
            for h in range(len(rows))
        ]
        for c in range(count)
    ]
    panel = []
    for h in range(len(rows)):
        own = (lane >= start) & (lane < start + count)
        unit = (lane == sub + (start + 8 * h)).astype(F32)
        panel.append(jnp.where(own, unit, rows[h]))
    done = [jnp.zeros((8, 128), F32) for _ in rows]
    for p in range(count):
        hp, sp = divmod(p, 8)
        pivot = jnp.broadcast_to(cols[p][hp][sp : sp + 1, :], (8, 128))
        scale = lax.rsqrt(pivot)
        line = jnp.broadcast_to(panel[hp][sp : sp + 1, :], (8, 128)) * scale
        done[hp] = jnp.where(sub == sp, line, done[hp])
        scaled = {}
        for h in range(hp, len(rows)):
            if h == hp:
                if sp == 7:
                    continue
                scaled[h] = jnp.where(sub > sp, cols[p][h] * scale, 0.0)
            else:
                scaled[h] = cols[p][h] * scale
        for h, f in scaled.items():
            panel[h] = panel[h] - f * line
        for c in range(p + 1, count):
            hc, sc = divmod(c, 8)
            head = jnp.broadcast_to(scaled[hc][sc : sc + 1, :], (8, 128))
            for h, f in scaled.items():
                if h >= hc:
                    cols[c][h] = cols[c][h] - f * head
    return done


def compress_kernel(panel_id, tiles, places, sends, grid, info, *refs):
    groups = 1 + max(g for g, _ in places.values())
    us, vs = refs[:groups], refs[groups : 2 * groups]
    parts = refs[2 * groups : 2 * groups + 4]
    (half, other, lp, upper, sketch) = refs[2 * groups + 4 : 2 * groups + 9]
    outs = refs[2 * groups + 9 : len(refs) - 10]
    (top, sk_t, turned, side, side_u, vl_t, nupd, sample, mat, inv) = refs[len(refs) - 10 :]
    row_place = info[0]
    col_place = info[1]
    n_row, n_col = grid
    first_core = info[8] == 0
    y = info[9]
    lefts = sorted({a for a, _ in tiles})
    tops = sorted({e for _, e in tiles})
    rank_width = sketch.shape[1]
    tile_size = sketch.shape[0]
    root_b = tile_size**0.5
    lane = lax.broadcasted_iota(jnp.int32, (8, 128), 1)
    sub = lax.broadcasted_iota(jnp.int32, (8, 128), 0)
    lane_row = lax.broadcasted_iota(jnp.int32, (1, 128), 1)

    def rank_of(a, e):
        return info[2 + a * 2 + e]

    def load(which, a, e):
        group, index = places[a, e]
        value = which[group][index]
        if panel_id == 0:
            value = value * (lane_row < rank_of(a, e)).astype(F32).astype(BF16)
        return value

    for k in range(4):
        turn = (k - y + 4) % 4
        near = jnp.where(turn == 0, parts[0][...], parts[1][...])
        far = jnp.where(turn == 2, parts[2][...], parts[3][...])
        if k % 2 in tops:
            top[k] = jnp.where(turn < 2, near, far)
    sk_t[...] = sketch[...].T
    for e in tops:
        turned[e] = dot_nn(lp[...], top[e]).astype(BF16)
    upper_t = upper[panel_id].T
    for a in lefts:
        side_u[a] = jnp.where(first_core, half[a], other[a])
        raw_v = jnp.where(first_core, other[a], half[a])
        wide = (dot_nn(upper_t, raw_v) * root_b).astype(BF16)
        side[a] = wide
        vl_t[a] = wide.T
    probe_top = {e: dot_nn(sk_t[...], top[2 + e]) for e in tops}

    for t, (a, e) in enumerate(tiles):
        coupling = (dot_nn(vl_t[a], turned[e]) * (1.0 / root_b)).astype(BF16)
        product = dot_nn(side_u[a], coupling)
        nupd[t] = (product * (-(rank_width**-0.5))).astype(BF16)
        probe_own = dot_nn(sk_t[...], load(vs, a, e))
        high, low = halves(jnp.concatenate([probe_own, probe_top[e]], axis=1))
        both = dot_nt(
            jnp.concatenate([load(us, a, e), nupd[t]], axis=1),
            jnp.concatenate([high, low], axis=0),
        )
        drawn = both[:, :rank_width] + both[:, rank_width:]
        drawn = jnp.where(lane_row < rank_of(a, e), drawn, 0.0)
        high, low = halves(drawn)
        sample[t] = jnp.concatenate([high, low], axis=1)
        gram = dot_tn(sample[t], sample[t])
        w = rank_width
        cross = gram[:w, w:]
        gram = (gram[:w, :w] + gram[w:, w:]) + (cross + gram[w:, :w])
        diag = lax.broadcasted_iota(jnp.int32, (w, w), 0)
        cols = lax.broadcasted_iota(jnp.int32, (w, w), 1)
        mat[t] = gram + jnp.where((diag == cols) & (cols >= rank_of(a, e)), 1.0, 0.0)

    def update(scaled):
        h, m, l = thirds(scaled)
        first = jnp.concatenate([h, h, m, m, h, l], axis=0)
        return first.T, jnp.concatenate([h, m, h, m, l, h], axis=0)

    for start in range(0, rank_width, STEP):
        stop = start + STEP
        for t in range(len(tiles)):
            rows = [mat[t, start + 8 * h : start + 8 * h + 8, :] for h in range(STEP // 8)]
            blocks = [row[:, start:stop] for row in rows]
            done = factor_block(rows, blocks, start, lane, sub)
            for h, piece in enumerate(done):
                inv[t, start + 8 * h : start + 8 * h + 8, :] = jnp.where(
                    lane < stop, piece, 0.0
                )
            if stop < rank_width:
                first, second = update(jnp.concatenate(done, axis=0))
                change = dot_nn(first[stop:, :], second)
                own = (lane_row >= start) & (lane_row < stop)
                mat[t, stop:, :] = jnp.where(own, 0.0, mat[t, stop:, :]) - change

    for t, (a, e) in enumerate(tiles):
        high, low = halves(inv[t])
        weights = jnp.concatenate(
            [
                jnp.concatenate([high, high], axis=1),
                jnp.concatenate([low, jnp.zeros_like(low)], axis=1),
            ],
            axis=0,
        )
        both = dot_nt(sample[t], weights)
        basis = both[:, :rank_width] + both[:, rank_width:]
        fresh_u = (basis * root_b).astype(BF16)
        keep_u = load(us, a, e)
        keep_v = load(vs, a, e)
        mixed = dot_tn(fresh_u, jnp.concatenate([keep_u, nupd[t]], axis=1))
        own_right = jnp.concatenate([keep_v, top[2 + e]], axis=1)
        if panel_id == PANELS - 1:
            right = dot_nt(own_right, mixed.astype(BF16))
        else:
            both = dot_nt(own_right, jnp.concatenate(halves(mixed), axis=0))
            right = both[:, :rank_width] + both[:, rank_width:]
        fresh_v = (right * (1.0 / tile_size)).astype(BF16)
        row_id = a * n_row + row_place
        col_id = e * n_col + col_place
        chosen = (row_id > panel_id) & (col_id > panel_id)
        settled = a * n_row > panel_id and e * n_col > panel_id
        if a == 0:
            keep_u = jnp.where((row_place == panel_id) & (col_id > panel_id), turned[e], keep_u)
        if e == 0:
            keep_v = jnp.where((col_place == panel_id) & (row_id > panel_id), side[a], keep_v)
        new_u = fresh_u if settled else jnp.where(chosen, fresh_u, keep_u)
        new_v = fresh_v if settled else jnp.where(chosen, fresh_v, keep_v)
        for value, spots in zip((new_u, new_v), sends[a, e]):
            for out, index in spots:
                outs[out][index] = value


def compress(
    panel_id, tiles, places, sends, depths, info, us, vs, parts, *shared
):
    count = len(tiles)
    size, width = shared[-1].shape
    vmem = pl.BlockSpec(memory_space=pltpu.VMEM)
    grid = (lax.axis_size(ROW), lax.axis_size(COL))
    flops = 2 * count * size * width * width * 30
    return pl.pallas_call(
        functools.partial(compress_kernel, panel_id, tiles, places, sends, grid),
        out_shape=[
            jax.ShapeDtypeStruct((depth,) * (depth > 0) + (size, width), BF16) for depth in depths
        ],
        in_specs=[pl.BlockSpec(memory_space=pltpu.SMEM)] + [vmem] * (2 * len(us) + 9),
        out_specs=[vmem] * len(depths),
        scratch_shapes=[
            pltpu.VMEM((4, size, width), BF16),
            pltpu.VMEM((width, size), BF16),
            pltpu.VMEM((2, size, width), BF16),
            pltpu.VMEM((3, size, width), BF16),
            pltpu.VMEM((3, size, width), BF16),
            pltpu.VMEM((3, width, size), BF16),
            pltpu.VMEM((count, size, width), BF16),
            pltpu.VMEM((count, size, 2 * width), BF16),
            pltpu.VMEM((count, width, width), F32),
            pltpu.VMEM((count, width, width), F32),
        ],
        compiler_params=pltpu.CompilerParams(vmem_limit_bytes=10 * 2**20),
        cost_estimate=pl.CostEstimate(
            flops=flops, bytes_accessed=8 * count * size * width, transcendentals=0
        ),
    )(info, *us, *vs, *parts, *shared)


ROW = ("y", "z")
COL = ("x", "core")


def spread_row(pieces, root):
    n_y, n_z = lax.axis_size("y"), lax.axis_size("z")
    y, z = lax.axis_index("y"), lax.axis_index("z")
    part = jnp.where((y == 0) & (z == root), pieces[0], 0)
    sent = [lax.ppermute(pieces[k], ROW, [(root, k * n_z + root)]) for k in range(1, n_y)]
    part = part + sent[0] + sent[1] + sent[2]

    def along_z(hops):
        pairs = [
            (k * n_z + (root + a) % n_z, k * n_z + (root + b) % n_z)
            for k in range(n_y)
            for a, b in hops
        ]
        return lax.ppermute(part, ROW, pairs)

    sent = [along_z([(0, 3)]), along_z([(0, 5)])]
    part = part + sent[0] + sent[1]
    sent = [along_z([(0, 1), (3, 4), (5, 6)]), along_z([(0, 7), (3, 2)])]
    part = part + sent[0] + sent[1]
    sent = [lax.ppermute(part, "y", [((k + s) % n_y, k) for k in range(n_y)]) for s in (2, 1, 3)]
    return [part, sent[1], sent[0], sent[2]]


def spread_col(side_u, side_v, root):
    n_core = lax.axis_size("core")
    x, core = lax.axis_index("x"), lax.axis_index("core")
    kept, given = (side_u, side_v) if root == 0 else (side_v, side_u)
    sent = lax.ppermute(given, COL, [(root, n_core - 1 - root)])
    start = jnp.where(x == 0, jnp.where(core == root, kept, sent), 0)
    sent = [lax.ppermute(start, "x", [(0, 1)]), lax.ppermute(start, "x", [(0, 3)])]
    half = start + sent[0] + sent[1]
    cut = half.shape[1] // 2
    low = lax.ppermute(half[:, :cut], "x", [(1, 2)])
    high = lax.ppermute(half[:, cut:], "x", [(3, 2)])
    half = half + jnp.concatenate([low, high], axis=1)
    other = lax.ppermute(half, "core", [(0, 1), (1, 0)])
    return half, other


ALL = ((0, 0), (0, 1), (1, 0), (1, 1), (2, 0), (2, 1))
WHOLE = Ellipsis


def on_device(tile_u, tile_v, tile_ranks, lower_inverse, upper_inverse, row_order, sketch):
    size, width = sketch.shape
    count = len(ALL)
    ranks = tile_ranks.reshape(count)
    keep = (jnp.arange(width, dtype=jnp.int32)[None, :] < ranks[:, None])[:, None, :]
    u = tile_u.reshape(count, size, width)
    v = tile_v.reshape(count, size, width)
    places = jnp.stack([lax.axis_index(ROW), lax.axis_index(COL)]).astype(jnp.int32)
    last = jnp.stack([lax.axis_index("core"), lax.axis_index("y")]).astype(jnp.int32)
    info = jnp.concatenate([places, ranks, last])
    spots = jnp.arange(size, dtype=jnp.int32)

    def turns(panel):
        pick = (row_order[panel][:, None] == spots[None, :]).astype(BF16)
        return dot_nn(lower_inverse[panel], pick).astype(BF16)

    pieces = [jnp.where(keep[n], x[n], 0) for x in (u, v) for n in (0, 1)]
    parts = spread_row(pieces, 0)
    half, other = spread_col(
        jnp.where(keep[0::2], u[0::2], 0), jnp.where(keep[0::2], v[0::2], 0), 0
    )
    flat = {tile: (0, n) for n, tile in enumerate(ALL)}
    shared = (parts, half, other, turns(0), upper_inverse, sketch)
    sends = {
        (0, 0): ([(0, WHOLE), (4, 0)], [(2, WHOLE), (5, 0)]),
        (0, 1): ([(1, WHOLE)], [(3, WHOLE)]),
        (1, 0): ([(4, 1)], [(5, 1)]),
        (2, 0): ([(4, 2)], [(5, 2)]),
        (1, 1): ([(6, 0)], [(7, 0)]),
        (2, 1): ([(6, 1)], [(7, 1)]),
    }
    *pieces, side_u, side_v, inner_u, inner_v = compress(
        0, ALL, flat, sends, (0, 0, 0, 0, 3, 3, 2, 2), info, (u,), (v,), *shared
    )
    parts = spread_row(pieces, 1)
    half, other = spread_col(side_u, side_v, 1)
    split = {
        (0, 0): (0, 0),
        (1, 0): (0, 1),
        (2, 0): (0, 2),
        (0, 1): (1, WHOLE),
        (1, 1): (2, 0),
        (2, 1): (2, 1),
    }
    sends = {tile: ([(0, n)], [(1, n)]) for n, tile in enumerate(ALL)}
    shared = (parts, half, other, turns(1), upper_inverse, sketch)
    ours = ((side_u, pieces[1], inner_u), (side_v, pieces[3], inner_v))
    u, v = compress(1, ALL, split, sends, (count, count), info, *ours, *shared)
    return u.reshape(tile_u.shape), v.reshape(tile_v.shape)


def solution(mesh):
    split = Mesh(mesh.devices.reshape(4, 8, 4, 2), ("y", "z", "x", "core"))
    tiles = P(None, ROW, None, COL, None, None)
    return jax.shard_map(
        on_device,
        mesh=split,
        in_specs=(tiles, tiles, P(None, ROW, None, COL), P(), P(), P(), P()),
        out_specs=(tiles, tiles),
        check_vma=False,
    )
```
